32 devices in a mesh: ctx: 8 (over z, x), head: 4 (over y, core).
Axes of the slice: x: 2, y: 2, z: 4, core: 2. Of those that a mesh axis runs over, the one named last changes fastest.
Arguments:
- queries: bfloat16 [4096, 4096], P('ctx', 'head'), may hold values from -5 to 5
- key_rows: bfloat16 [4096, 1024], P('ctx', 'head'), may hold values from -5 to 5
- value_rows: bfloat16 [4096, 1024], P('ctx', 'head'), may hold values from -6 to 6
- slash_offsets: int32 [32, 4], P('head'), may hold values from 0 to 8, as said below
- union_blocks: int32 [8, 8, 2], P('head'), may hold values from 0 to 7, as said below
- head_picks: int32 [32, 8, 1], P('head'), may hold values from 0 to 1, as said below
- owner_counts: int32 [32, 8], P('head'), may hold values from 0 to 1, as said below
- out_weight: bfloat16 [4096, 4096], P(None, 'head'), may hold values from -0.09375 to 0.09375
Outputs:
- projected: bfloat16 [4096, 4096], P('ctx', 'head')
The draws below stay inside these ranges and needn't reach their ends.
Inputs may be any that keep to these rules, and one draw needn't show every extreme that they name: `slash_offsets`: each head's offsets are distinct and include 0 and 8. `union_blocks`: the 2 entries of each KV head and sequence block are distinct. `head_picks`: the 1 entries of each query head and sequence block are distinct. `owner_counts`: equal to 1 for sequence block 0.
All inputs are finite; a program needn't handle non-finite values.
Results may differ from the reference program's by a relative error of at most 0.0056.
Values may be sent and summed in bfloat16 or wider, within the bound.
No kernel may reach another device: no remote copies, remote signals or barrier semaphores. Data moves between devices by JAX's collectives and lax.ppermute only.
A program may use at most 128 MiB of HBM per device.

```python
import jax
import jax.numpy as jnp
from jax import lax

D = 4096
HQ = 32
KVH = 8
HEAD_SIZE = 128
BLOCK_TOKENS = 64
NS = 4
VPER = 1
UNION = 2
TOK_DEV = 512
SEQ = 4096


def paired_draw(key):
    base_key = jax.random.fold_in(key, 7)
    keys_list = jax.random.split(base_key, 2)
    query_draw = jax.random.truncated_normal(keys_list[0], -4.5, 4.5, (SEQ, HQ * HEAD_SIZE), jnp.float32)
    key_draw = jax.random.truncated_normal(keys_list[1], -4.5, 4.5, (SEQ, KVH * HEAD_SIZE), jnp.float32)
    return (query_draw, key_draw)


def draw_queries(key, part):
    return paired_draw(key)[0].astype(jnp.bfloat16)


def draw_key_rows(key, part):
    return paired_draw(key)[1].astype(jnp.bfloat16)


def distinct_order(key, shape):
    width = shape[-1]
    scores = jax.random.randint(key, shape, 0, 65536) * width + jnp.arange(width, dtype=jnp.int32)
    return jnp.argsort(scores, axis=-1, stable=True).astype(jnp.int32)


def draw_slash_offsets(key, part):
    reach = TOK_DEV // BLOCK_TOKENS
    orders = distinct_order(jax.random.fold_in(key, 3), (HQ, reach - 1))
    middle = orders[:, :NS - 2] + 1
    first = jnp.zeros((HQ, 1), jnp.int32)
    farthest = jnp.full((HQ, 1), reach, jnp.int32)
    return jnp.concatenate([first, farthest, middle], axis=1).astype(jnp.int32)


def draw_union_blocks(key, part):
    orders = distinct_order(jax.random.fold_in(key, 5), (KVH, SEQ // TOK_DEV, TOK_DEV // BLOCK_TOKENS))
    return orders[:, :, :UNION]


def draw_head_picks(key, part):
    orders = distinct_order(jax.random.fold_in(key, 9), (HQ, SEQ // TOK_DEV, UNION))
    return orders[:, :, :VPER]


def draw_owner_counts(key, part):
    counts = jax.random.randint(jax.random.fold_in(key, 13), (HQ, SEQ // TOK_DEV), 0, VPER + 1)
    return counts.at[:, 0].set(VPER).astype(jnp.int32)


def block_scale(own_key, dims, pieces, least, largest):
    factor_of, own = 1.0, jax.random.fold_in(own_key, 6)
    for axis_at, shards_of in pieces:
        draws = jnp.exp(jax.random.uniform(jax.random.fold_in(own, axis_at), (shards_of,), jnp.float32, least / len(pieces), largest / len(pieces)))
        factor_of = factor_of * jnp.repeat(draws, dims[axis_at] // shards_of).reshape([-1 if axis == axis_at else 1 for axis in range(len(dims))])
    return factor_of


def bell_draw(rng, dims, spread, most, shards=(), kind=jnp.bfloat16):
    result = spread * jax.random.normal(rng, dims, jnp.float32)
    if shards:
        result = result * block_scale(rng, dims, shards, -0.22, 0.18)
    return jnp.clip(result, -most, most).astype(kind)


def setup_inputs(seed: int = 0) -> dict:
    key_list = jax.random.split(jax.random.key(seed), 9)
    return {
        "queries": draw_queries(jax.random.fold_in(key_list[8], 71), 0),
        "key_rows": draw_key_rows(jax.random.fold_in(key_list[8], 71), 0),
        "value_rows": bell_draw(key_list[2], (SEQ, KVH * HEAD_SIZE), 1.0, 6.0, ((0, 8), (1, 4))),
        "slash_offsets": draw_slash_offsets(jax.random.fold_in(key_list[8], 71), 0),
        "union_blocks": draw_union_blocks(jax.random.fold_in(key_list[8], 71), 0),
        "head_picks": draw_head_picks(jax.random.fold_in(key_list[8], 71), 0),
        "owner_counts": draw_owner_counts(jax.random.fold_in(key_list[8], 71), 0),
        "out_weight": bell_draw(key_list[7], (HQ * HEAD_SIZE, D), (HQ * HEAD_SIZE) ** -0.5, 0.09375, ((1, 4),)),
    }


def attend(vert_scores, vert_mask, diagonal_scores, slash_mask, vert_values, diagonal_values, count_of_blocks):
    masked_vert = jnp.where(vert_mask, vert_scores, -1e30)
    masked_slash = jnp.where(slash_mask, diagonal_scores, -1e30)
    peak = jnp.maximum(jnp.max(masked_vert, axis=-1, keepdims=True), jnp.max(masked_slash, axis=-1, keepdims=True))
    weight_vert = jnp.exp(masked_vert - peak)
    weight_slash = jnp.exp(masked_slash - peak)
    total = jnp.sum(weight_vert, axis=-1, keepdims=True) + jnp.sum(weight_slash, axis=-1, keepdims=True)
    prob_vert = weight_vert.astype(jnp.bfloat16)
    slash_probability = lax.optimization_barrier(weight_slash.astype(jnp.bfloat16)).astype(jnp.float32)
    numer = jnp.dot(prob_vert, vert_values, preferred_element_type=jnp.float32)
    slash_probability = slash_probability.reshape(count_of_blocks, BLOCK_TOKENS, NS, BLOCK_TOKENS)
    diagonal_portion = jnp.einsum("wojf,wjfl->wol", slash_probability, diagonal_values.astype(jnp.float32), precision=lax.Precision.HIGHEST)
    numer = numer + diagonal_portion.reshape(count_of_blocks * BLOCK_TOKENS, HEAD_SIZE)
    return (numer / total).astype(jnp.bfloat16)


def reference(queries, key_rows, value_rows, slash_offsets, union_blocks, head_picks, owner_counts, out_weight):
    group_size = HQ // KVH
    per_dev = TOK_DEV // BLOCK_TOKENS
    count_of_blocks = SEQ // BLOCK_TOKENS
    scale_of_scores = jnp.float32(HEAD_SIZE ** -0.5)
    inner_offset = jnp.arange(BLOCK_TOKENS, dtype=jnp.int32)
    query_place = jnp.arange(SEQ, dtype=jnp.int32)
    query_block = jnp.arange(count_of_blocks, dtype=jnp.int32)
    owner_base = jnp.arange(SEQ // TOK_DEV, dtype=jnp.int32)[:, None] * per_dev
    query_all = queries.reshape(SEQ, HQ, HEAD_SIZE)
    key_all = key_rows.reshape(SEQ, KVH, HEAD_SIZE)
    value_all = value_rows.reshape(SEQ, KVH, HEAD_SIZE)

    def one_head(head_index):
        kv_index = (head_index // group_size).astype(jnp.int32)
        query_head = lax.dynamic_index_in_dim(query_all, head_index, 1, keepdims=False)
        key_head = lax.dynamic_index_in_dim(key_all, kv_index, 1, keepdims=False)
        value_head = lax.dynamic_index_in_dim(value_all, kv_index, 1, keepdims=False)
        offsets = lax.dynamic_index_in_dim(slash_offsets, head_index, 0, keepdims=False)
        unions = lax.dynamic_index_in_dim(union_blocks, kv_index, 0, keepdims=False)
        picks = lax.dynamic_index_in_dim(head_picks, head_index, 0, keepdims=False)
        counts = lax.dynamic_index_in_dim(owner_counts, head_index, 0, keepdims=False)
        blocks_flat = (owner_base + jnp.take_along_axis(unions, picks, axis=1)).reshape(-1).astype(jnp.int32)
        valid_flat = (jnp.arange(VPER, dtype=jnp.int32)[None, :] < counts[:, None]).reshape(-1)
        slot_count = blocks_flat.shape[0]
        key_blocks = key_head.reshape(count_of_blocks, BLOCK_TOKENS, HEAD_SIZE)
        value_blocks = value_head.reshape(count_of_blocks, BLOCK_TOKENS, HEAD_SIZE)
        vert_keys = key_blocks[blocks_flat].reshape(slot_count * BLOCK_TOKENS, HEAD_SIZE)
        vert_values = value_blocks[blocks_flat].reshape(slot_count * BLOCK_TOKENS, HEAD_SIZE)
        query_single_float = query_head.astype(jnp.float32)
        vert_scores = jnp.einsum("qd,kd->qk", query_single_float, vert_keys.astype(jnp.float32), precision=lax.Precision.HIGHEST) * scale_of_scores
        distance = query_block[:, None] - blocks_flat[None, :]
        on_slash = jnp.any(distance[:, :, None] == offsets[None, None, :], axis=2)
        block_mask = valid_flat[None, :] & jnp.logical_not(on_slash)
        key_place = (blocks_flat[:, None] * BLOCK_TOKENS + inner_offset[None, :]).reshape(-1)
        vert_mask = jnp.broadcast_to(block_mask[:, None, :, None], (count_of_blocks, BLOCK_TOKENS, slot_count, BLOCK_TOKENS)).reshape(SEQ, slot_count * BLOCK_TOKENS)
        vert_mask = vert_mask & (key_place[None, :] <= query_place[:, None])
        slash_index = query_block[:, None] - offsets[None, :]
        slash_valid = slash_index >= 0
        slash_block = jnp.maximum(slash_index, 0).astype(jnp.int32)
        diagonal_keys = key_blocks[slash_block]
        diagonal_values = value_blocks[slash_block]
        diagonal_scores = jnp.einsum("hax,hisx->hais", query_single_float.reshape(count_of_blocks, BLOCK_TOKENS, HEAD_SIZE), diagonal_keys.astype(jnp.float32), precision=lax.Precision.HIGHEST) * scale_of_scores
        slash_mask = slash_valid[:, None, :, None] & ((offsets[None, None, :, None] > 0) | (inner_offset[None, None, None, :] <= inner_offset[None, :, None, None]))
        slash_mask = jnp.broadcast_to(slash_mask, (count_of_blocks, BLOCK_TOKENS, NS, BLOCK_TOKENS)).reshape(SEQ, NS * BLOCK_TOKENS)
        return attend(vert_scores, vert_mask, diagonal_scores.reshape(SEQ, NS * BLOCK_TOKENS), slash_mask, vert_values, diagonal_values, count_of_blocks)

    per_head = lax.map(one_head, jnp.arange(HQ, dtype=jnp.int32))
    attended = per_head.transpose(1, 0, 2).reshape(SEQ, HQ * HEAD_SIZE)
    return jnp.dot(attended, out_weight, preferred_element_type=jnp.float32).astype(jnp.bfloat16)
```

```python
import functools

import jax
import jax.numpy as jnp
from jax import lax
from jax.experimental import pallas as pl
from jax.experimental.pallas import tpu as pltpu
from jax.sharding import PartitionSpec as P


HEAD_SIZE = 128
BLOCK = 64
PAIR = 2 * BLOCK
LOG2E = 1.4426950408889634
SCALE2 = HEAD_SIZE**-0.5 * LOG2E
HIDE = -1e30
CONTRACT = (((1,), (1,)), ((), ()))


def prep_body(unions, keys, values, *outs, groups, union):
    rank = lax.axis_index("ctx")
    blocks = outs[groups]
    for g in range(groups):
        cols = pl.ds(g * HEAD_SIZE, HEAD_SIZE)
        outs[g][:, :HEAD_SIZE] = keys[:, cols]
        outs[g][:, HEAD_SIZE:] = values[:, cols]
        for u in range(union):
            start = pl.multiple_of(unions[g, rank, u] * BLOCK, BLOCK)
            rows = pl.ds((g * union + u) * BLOCK, BLOCK)
            blocks[rows, :HEAD_SIZE] = keys[pl.ds(start, BLOCK), cols]
            blocks[rows, HEAD_SIZE:] = values[pl.ds(start, BLOCK), cols]


def smem():
    return pl.BlockSpec(memory_space=pltpu.SMEM)


def vmem():
    return pl.BlockSpec(memory_space=pltpu.VMEM)


def prep(unions, keys, values, groups, union):
    tokens = keys.shape[0]
    wide = 2 * HEAD_SIZE
    return pl.pallas_call(
        functools.partial(prep_body, groups=groups, union=union),
        out_shape=[jax.ShapeDtypeStruct((tokens, wide), keys.dtype)] * groups
        + [jax.ShapeDtypeStruct((groups * union * BLOCK, wide), keys.dtype)],
        grid=(1,),
        in_specs=[smem()] + [pl.BlockSpec(keys.shape, lambda p: (0, 0))] * 2,
        out_specs=[vmem()] * (groups + 1),
        compiler_params=pltpu.CompilerParams(vmem_limit_bytes=8 << 20),
        name="prep",
    )(unions, keys, values)


def picked(picks, counts, head, owner, j):
    return picks[head, owner, j], j < counts[head, owner]


def near_body(
    offsets_ref, unions, picks, counts, q_ref, prev_ref, local_ref, sum_ref, peak_ref, total_ref, window,
    *, group, heads, per_dev,
):
    rank = lax.axis_index("ctx")
    tokens = per_dev * BLOCK
    wide = (per_dev + 2) * BLOCK
    window[:tokens, :] = prev_ref[...]
    window[tokens:, :] = local_ref[...]
    place = lax.broadcasted_iota(jnp.int32, (1, wide), 1) // BLOCK
    row = lax.broadcasted_iota(jnp.int32, (PAIR, PAIR), 0)
    col = lax.broadcasted_iota(jnp.int32, (PAIR, PAIR), 1)
    causal = jnp.where(row >= col, 0.0, HIDE)

    def scores_of(step):
        rows = slice(step * PAIR, (step + 1) * PAIR)
        queries = [q_ref[rows, i * HEAD_SIZE : (i + 1) * HEAD_SIZE] for i in range(heads)]
        return lax.dot_general(
            jnp.concatenate(queries, axis=0), window[step * PAIR : step * PAIR + wide, :HEAD_SIZE], CONTRACT,
            preferred_element_type=jnp.float32,
        )

    slashes, columns = [], []
    for i in range(heads):
        head = group * heads + i
        slashes.append([offsets_ref[head, s] for s in range(offsets_ref.shape[1])])
        at = []
        for j in range(picks.shape[2]):
            entry, used = picked(picks, counts, head, rank, j)
            at.append(jnp.where(used, unions[group, rank, entry] + per_dev, -tokens))
        columns.append(at)
    seen_slash = []
    for i in range(heads):
        for half in range(2):
            distance = half + per_dev - place
            seen = distance == slashes[i][0]
            for offset in slashes[i][1:]:
                seen = seen | (distance == offset)
            seen_slash.append((distance, jnp.where(seen, 0.0, HIDE)))

    steps = tokens // PAIR
    ahead = scores_of(0)
    for step in range(steps):
        near = ahead
        if step + 1 < steps:
            ahead = scores_of(step + 1)
        exists = place + (rank * per_dev - per_dev + 2 * step) >= 0
        parts = []
        for i in range(heads):
            for half in range(2):
                distance, bias = seen_slash[2 * i + half]
                for column in columns[i]:
                    bias = jnp.where((place == column - 2 * step) & (distance > 0), 0.0, bias)
                begin = i * PAIR + half * BLOCK
                piece = near[begin : begin + BLOCK] + jnp.where(exists, bias, HIDE)
                triangle = causal[half * BLOCK : (half + 1) * BLOCK]
                parts.append(
                    jnp.concatenate([piece[:, : wide - PAIR], piece[:, wide - PAIR :] + triangle], axis=1)
                )
        near = jnp.concatenate(parts, axis=0)
        peak = jnp.max(near, axis=1, keepdims=True)
        weight = jnp.exp2((near - peak) * SCALE2)
        total = jnp.sum(weight, axis=1, keepdims=True)
        sums = jnp.dot(
            weight.astype(jnp.bfloat16), window[step * PAIR : step * PAIR + wide, HEAD_SIZE:],
            preferred_element_type=jnp.float32,
        )
        out = slice(step * PAIR, (step + 1) * PAIR)
        for i in range(heads):
            rows = slice(i * PAIR, (i + 1) * PAIR)
            cols = slice(i * HEAD_SIZE, (i + 1) * HEAD_SIZE)
            sum_ref[out, cols] = sums[rows]
            peak_ref[out, cols] = jnp.broadcast_to(peak[rows], (PAIR, HEAD_SIZE))
            total_ref[out, cols] = jnp.broadcast_to(total[rows], (PAIR, HEAD_SIZE))


def attend_near(scalars, queries, prev, local, group, heads):
    tokens = queries.shape[0]
    cols = heads * HEAD_SIZE
    return pl.pallas_call(
        functools.partial(near_body, group=group, heads=heads, per_dev=tokens // BLOCK),
        grid=(1,),
        out_shape=[jax.ShapeDtypeStruct((tokens, cols), jnp.float32)] * 3,
        in_specs=[smem()] * 4 + [pl.BlockSpec((tokens, cols), lambda p: (0, group)), vmem(), vmem()],
        out_specs=[vmem()] * 3,
        scratch_shapes=[pltpu.VMEM((2 * tokens, 2 * HEAD_SIZE), queries.dtype)],
        compiler_params=pltpu.CompilerParams(vmem_limit_bytes=16 << 20),
        cost_estimate=pl.CostEstimate(
            flops=4 * tokens * cols * 640 * 3, transcendentals=tokens * heads * 640, bytes_accessed=4 * tokens * cols
        ),
    )(*scalars, queries, prev, local)


def far_body(
    offsets_ref, unions, picks, counts, q_ref, sum_ref, peak_ref, total_ref, prev_ref, same_ref, other_ref, out_ref, far,
    *, group, heads, per_dev, owners,
):
    rank = lax.axis_index("ctx")
    vper, union = picks.shape[2], unions.shape[2]
    hops = owners // 2 - 1
    slots = [(None, 0, j) for j in range(vper)]
    slots += [(k, side, j) for k in range(hops) for side in range(2) for j in range(vper)]
    extra = len(slots) % 2
    slots += [slots[-1]] * extra
    lane = lax.broadcasted_iota(jnp.int32, (1, PAIR), 1)
    block_row = lax.broadcasted_iota(jnp.int32, (per_dev, PAIR), 0)

    hides = []
    for i in range(heads):
        head = group * heads + i
        goods = []
        for at, slot in enumerate(slots):
            k, side, j = slot
            owner = rank - 1 if k is None else (rank ^ 1 if side else rank) - 2 * (k + 1)
            good = (owner >= 0) & (owner <= rank - (1 if k is None else 2))
            owner = jnp.maximum(owner, 0)
            entry, used = picked(picks, counts, head, owner, j)
            good = good & used
            if extra and at == len(slots) - 1:
                good = good & False
            if k is None:
                source = prev_ref
                block = unions[group, owner, entry]
                distance = block_row + (per_dev - block)
                seen = jnp.full((per_dev, PAIR), 1.0)
                for s in range(offsets_ref.shape[1]):
                    seen = jnp.where(distance == offsets_ref[head, s], 0.0, seen)
                bias = jnp.where(seen * jnp.where(good, 1.0, 0.0) > 0.5, 0.0, HIDE)
                start = block * BLOCK
            else:
                source = other_ref if side else same_ref
                bias = jnp.where(good, 0.0, HIDE).astype(jnp.float32)
                start = (k * union + entry) * BLOCK
            goods.append(bias)
            far[i, pl.ds(at * BLOCK, BLOCK), :] = source[pl.ds(pl.multiple_of(start, BLOCK), BLOCK), :]
        masks = []
        for tile in range(len(slots) // 2):
            mask = jnp.where(lane < BLOCK, goods[2 * tile], goods[2 * tile + 1])
            if mask.shape[0] > 1:
                mask = jnp.concatenate(
                    [jnp.broadcast_to(mask[r : r + 1], (BLOCK, PAIR)) for r in range(per_dev)], axis=0
                )
            masks.append(mask)
        hides.append(masks)

    def scores_of(i):
        return lax.dot_general(
            q_ref[:, i * HEAD_SIZE : (i + 1) * HEAD_SIZE], far[i, :, :HEAD_SIZE], CONTRACT,
            preferred_element_type=jnp.float32,
        )

    ahead = scores_of(0)
    for i in range(heads):
        cols = slice(i * HEAD_SIZE, (i + 1) * HEAD_SIZE)
        scores = ahead
        if i + 1 < heads:
            ahead = scores_of(i + 1)
        tiles = [scores[:, t * PAIR : (t + 1) * PAIR] + mask for t, mask in enumerate(hides[i])]
        before = peak_ref[:, cols]
        highest = functools.reduce(jnp.maximum, tiles)
        peak = jnp.maximum(jnp.max(highest, axis=1, keepdims=True), before)
        weights = [jnp.exp2((tile - peak) * SCALE2) for tile in tiles]
        keep = jnp.exp2((before - peak) * SCALE2)
        total = jnp.sum(functools.reduce(jnp.add, weights), axis=1, keepdims=True) + keep * total_ref[:, cols]
        numer = jnp.dot(
            jnp.concatenate([w.astype(jnp.bfloat16) for w in weights], axis=1), far[i, :, HEAD_SIZE:],
            preferred_element_type=jnp.float32,
        )
        out_ref[:, cols] = ((numer + keep * sum_ref[:, cols]) / total).astype(out_ref.dtype)


def attend_far(scalars, queries, sums, peaks, totals, prev, same, other, group, heads, owners):
    tokens = queries.shape[0]
    cols = heads * HEAD_SIZE
    slots = (owners - 1) * scalars[2].shape[2]
    slots += slots % 2
    per_dev = tokens // BLOCK
    return pl.pallas_call(
        functools.partial(far_body, group=group, heads=heads, per_dev=per_dev, owners=owners),
        grid=(1,),
        out_shape=jax.ShapeDtypeStruct((tokens, cols), queries.dtype),
        in_specs=[smem()] * 4 + [pl.BlockSpec((tokens, cols), lambda p: (0, group))] + [vmem()] * 6,
        out_specs=vmem(),
        scratch_shapes=[
            pltpu.VMEM((heads, slots * BLOCK, 2 * HEAD_SIZE), queries.dtype),
        ],
        compiler_params=pltpu.CompilerParams(vmem_limit_bytes=24 << 20),
        cost_estimate=pl.CostEstimate(
            flops=4 * tokens * cols * 512 * 3, transcendentals=tokens * heads * 512, bytes_accessed=4 * tokens * cols
        ),
    )(*scalars, queries, sums, peaks, totals, prev, same, other)


def project_body(*refs, spots, has_sum, groups):
    count = len(spots)
    ins, weight = refs[:count], refs[count]
    out = refs[-1]
    seat, members = lax.axis_index("head"), lax.axis_size("head")
    depth = ins[0].shape[1]
    total = refs[count + 1][...] if has_sum else None
    for x, (flip, by, g) in zip(ins, spots):
        source = lax.rem((seat ^ 1 if flip else seat) + members - by, members)
        start = pl.multiple_of((source * groups + g) * depth, depth)
        part = jnp.dot(x[...], weight[pl.ds(start, depth), :], preferred_element_type=jnp.float32)
        total = part if total is None else total + part
    out[...] = total.astype(out.dtype)


def project(ins, spots, weight, sums, dtype, groups):
    tokens, depth = ins[0].shape
    cols = weight.shape[1]
    args = list(ins) + [weight] + ([] if sums is None else [sums])
    return pl.pallas_call(
        functools.partial(project_body, spots=spots, has_sum=sums is not None, groups=groups),
        in_specs=[vmem()] * len(args),
        out_specs=vmem(),
        out_shape=jax.ShapeDtypeStruct((tokens, cols), dtype),
        compiler_params=pltpu.CompilerParams(vmem_limit_bytes=24 << 20),
        cost_estimate=pl.CostEstimate(
            flops=2 * tokens * cols * depth * len(ins) * 2, transcendentals=0, bytes_accessed=2 * depth * cols * len(ins)
        ),
    )(*args)


def turn(array, axis, by):
    size = lax.axis_size(axis)
    return lax.ppermute(array, axis, [(i, (i + by) % size) for i in range(size)])


def onward(array, axis, by):
    size = lax.axis_size(axis)
    return lax.ppermute(array, axis, [(i, i + by) for i in range(size - by)])


def swap(array, axis):
    size = lax.axis_size(axis)
    return lax.ppermute(array, axis, [(i, i ^ 1) for i in range(size)])


def shards(
    queries, key_rows, value_rows, slash_offsets, union_blocks, head_picks, owner_counts, out_weight
):
    groups = key_rows.shape[1] // HEAD_SIZE
    owners, members = lax.axis_size("ctx"), lax.axis_size("head")
    heads = slash_offsets.shape[0] // groups
    scalars = (slash_offsets, union_blocks, head_picks, owner_counts)
    made = prep(union_blocks, key_rows, value_rows, groups, union_blocks.shape[2])
    joined, blocks = made[:groups], made[groups]
    hops = owners // 2 - 1
    prevs, near, sames, others = [], [], [], []
    arrived = []
    for k in reversed(range(hops)):
        arrived.append(onward(blocks, "ctx", 2 * (k + 1)))
    span = blocks.shape[0] // groups
    for g in range(groups):
        rows = slice(g * span, (g + 1) * span)
        prevs.append(onward(joined[g], "ctx", 1))
        if hops > 0:
            sames.append(jnp.concatenate([part[rows] for part in arrived[::-1]], axis=0))
            others.append(swap(sames[g], "ctx"))
        else:
            sames.append(blocks[rows])
            others.append(blocks[rows])
    for g in range(groups):
        near.append(attend_near(scalars, queries, prevs[g], joined[g], g, heads))
    done, mates = [], []
    for g in range(groups):
        done.append(attend_far(scalars, queries, *near[g], prevs[g], sames[g], others[g], g, heads, owners))
        mates.append(swap(done[g], "head"))
    sums = None
    crossed = []
    for by in range(2, members, 2):
        for g in range(groups):
            here = turn(done[g], "head", by)
            crossed.append((here, swap(here, "head"), by, g))
    for g in range(groups):
        only = not crossed and g == groups - 1
        sums = project(
            [done[g], mates[g]], [(False, 0, g), (True, 0, g)], out_weight, sums,
            jnp.bfloat16 if only else jnp.float32, groups,
        )
    for at, (here, there, by, g) in enumerate(crossed):
        last = at == len(crossed) - 1
        sums = project([here], [(False, by, g)], out_weight, sums, jnp.float32, groups)
        sums = project([there], [(True, by, g)], out_weight, sums, jnp.bfloat16 if last else jnp.float32, groups)
    return sums


def solution(mesh):
    in_specs = (
        P("ctx", "head"),
        P("ctx", "head"),
        P("ctx", "head"),
        P("head", None),
        P("head", None, None),
        P("head", None, None),
        P("head", None),
        P(None, "head"),
    )
    return jax.shard_map(shards, mesh=mesh, in_specs=in_specs, out_specs=P("ctx", "head"), check_vma=False)
```

```python
import functools

import jax
import jax.numpy as jnp
from jax import lax
from jax.experimental import pallas as pl
from jax.experimental.pallas import tpu as pltpu
from jax.sharding import PartitionSpec as P


HEAD_SIZE = 128
BLOCK = 64
PAIR = 2 * BLOCK
LOG2E = 1.4426950408889634
SCALE2 = HEAD_SIZE**-0.5 * LOG2E
HIDE = -1e30
CONTRACT = (((1,), (1,)), ((), ()))


def prep_body(unions_hbm, keys_hbm, values_hbm, *outs, groups, union):
    *outs, unions, keys, values, sems = outs
    loads = [
        pltpu.make_async_copy(unions_hbm, unions, sems.at[2]),
        pltpu.make_async_copy(keys_hbm, keys, sems.at[0]),
        pltpu.make_async_copy(values_hbm, values, sems.at[1]),
    ]
    for load in loads:
        load.start()
    for load in loads:
        load.wait()
    rank = lax.axis_index("ctx")
    for g in range(groups):
        blocks = outs[groups + g]
        cols = pl.ds(g * HEAD_SIZE, HEAD_SIZE)
        outs[g][:, :HEAD_SIZE] = keys[:, cols]
        outs[g][:, HEAD_SIZE:] = values[:, cols]
        for u in range(union):
            start = pl.multiple_of(unions[g, u, rank] * BLOCK, BLOCK)
            rows = pl.ds(u * BLOCK, BLOCK)
            every = pl.ds((g * union + u) * BLOCK, BLOCK)
            for block_out, at in ((blocks, rows), (outs[2 * groups], every)):
                block_out[at, :HEAD_SIZE] = keys[pl.ds(start, BLOCK), cols]
                block_out[at, HEAD_SIZE:] = values[pl.ds(start, BLOCK), cols]


def hbm():
    return pl.BlockSpec(memory_space=pltpu.HBM)


def stay(array):
    return pltpu.with_memory_space_constraint(array, pltpu.HBM)


def small(arrays):
    return [pltpu.SMEM(a.shape, a.dtype) for a in arrays]


def vmem():
    return pl.BlockSpec(memory_space=pltpu.VMEM)


def prep(unions, keys, values, groups, union):
    tokens = keys.shape[0]
    wide = 2 * HEAD_SIZE
    return pl.pallas_call(
        functools.partial(prep_body, groups=groups, union=union),
        out_shape=[jax.ShapeDtypeStruct((tokens, wide), keys.dtype)] * groups
        + [jax.ShapeDtypeStruct((union * BLOCK, wide), keys.dtype)] * groups
        + [jax.ShapeDtypeStruct((groups * union * BLOCK, wide), keys.dtype)],
        in_specs=[hbm()] * 3,
        out_specs=[vmem()] * (2 * groups + 1),
        scratch_shapes=small([unions]) + [pltpu.VMEM(keys.shape, keys.dtype)] * 2 + [pltpu.SemaphoreType.DMA((3,))],
        compiler_params=pltpu.CompilerParams(vmem_limit_bytes=8 << 20),
        name="prep",
    )(stay(unions), stay(keys), stay(values))


def picked(picks, counts, head, owner, j):
    return picks[head, j, owner], j < counts[head, owner]


def near_body(
    offsets_hbm, unions_hbm, picks_hbm, counts_hbm, q_hbm, prev_ref, local_ref, sum_ref, peak_ref, total_ref, window,
    q_ref, offsets_ref, unions, picks, counts, sem,
    *, group, heads, per_dev,
):
    rank = lax.axis_index("ctx")
    tokens = per_dev * BLOCK
    wide = (per_dev + 2) * BLOCK
    width = heads * HEAD_SIZE
    load = pltpu.make_async_copy(q_hbm.at[:, pl.ds(group * width, width)], q_ref, sem.at[4])
    load.start()
    tables = [(offsets_hbm, offsets_ref), (unions_hbm, unions), (picks_hbm, picks), (counts_hbm, counts)]
    tables = [pltpu.make_async_copy(a, b, sem.at[i]) for i, (a, b) in enumerate(tables)]
    for copy in tables:
        copy.start()
    window[:tokens, :] = prev_ref[...]
    window[tokens:, :] = local_ref[...]
    place = lax.broadcasted_iota(jnp.int32, (1, wide), 1) // BLOCK
    row = lax.broadcasted_iota(jnp.int32, (PAIR, PAIR), 0)
    col = lax.broadcasted_iota(jnp.int32, (PAIR, PAIR), 1)
    causal = jnp.where(row >= col, 0.0, HIDE)

    def scores_of(step):
        rows = slice(step * PAIR, (step + 1) * PAIR)
        queries = [q_ref[rows, i * HEAD_SIZE : (i + 1) * HEAD_SIZE] for i in range(heads)]
        return lax.dot_general(
            jnp.concatenate(queries, axis=0), window[step * PAIR : step * PAIR + wide, :HEAD_SIZE], CONTRACT,
            preferred_element_type=jnp.float32,
        )

    for copy in tables:
        copy.wait()
    slashes, columns = [], []
    for i in range(heads):
        head = group * heads + i
        slashes.append([offsets_ref[s, head] for s in range(offsets_ref.shape[0])])
        at = []
        for j in range(picks.shape[1]):
            entry, used = picked(picks, counts, head, rank, j)
            at.append(jnp.where(used, unions[group, entry, rank] + per_dev, -tokens))
        columns.append(at)
    seen_slash = []
    for i in range(heads):
        for half in range(2):
            distance = half + per_dev - place
            seen = distance == slashes[i][0]
            for offset in slashes[i][1:]:
                seen = seen | (distance == offset)
            seen_slash.append((distance, jnp.where(seen, 0.0, HIDE)))

    steps = tokens // PAIR
    load.wait()
    ahead = scores_of(0)
    for step in range(steps):
        near = ahead
        if step + 1 < steps:
            ahead = scores_of(step + 1)
        exists = place + (rank * per_dev - per_dev + 2 * step) >= 0
        parts = []
        for i in range(heads):
            for half in range(2):
                distance, bias = seen_slash[2 * i + half]
                for column in columns[i]:
                    bias = jnp.where((place == column - 2 * step) & (distance > 0), 0.0, bias)
                begin = i * PAIR + half * BLOCK
                piece = near[begin : begin + BLOCK] + jnp.where(exists, bias, HIDE)
                triangle = causal[half * BLOCK : (half + 1) * BLOCK]
                parts.append(
                    jnp.concatenate([piece[:, : wide - PAIR], piece[:, wide - PAIR :] + triangle], axis=1)
                )
        near = jnp.concatenate(parts, axis=0)
        peak = jnp.max(near, axis=1, keepdims=True)
        weight = jnp.exp2((near - peak) * SCALE2)
        total = jnp.sum(weight, axis=1, keepdims=True)
        sums = jnp.dot(
            weight.astype(jnp.bfloat16), window[step * PAIR : step * PAIR + wide, HEAD_SIZE:],
            preferred_element_type=jnp.float32,
        )
        out = slice(step * PAIR, (step + 1) * PAIR)
        for i in range(heads):
            rows = slice(i * PAIR, (i + 1) * PAIR)
            cols = slice(i * HEAD_SIZE, (i + 1) * HEAD_SIZE)
            sum_ref[out, cols] = sums[rows]
            peak_ref[out, cols] = jnp.broadcast_to(peak[rows], (PAIR, HEAD_SIZE))
            total_ref[out, cols] = jnp.broadcast_to(total[rows], (PAIR, HEAD_SIZE))


def attend_near(scalars, queries, prev, local, group, heads):
    tokens = queries.shape[0]
    cols = heads * HEAD_SIZE
    return pl.pallas_call(
        functools.partial(near_body, group=group, heads=heads, per_dev=tokens // BLOCK),
        out_shape=[jax.ShapeDtypeStruct((tokens, cols), jnp.float32)] * 3,
        in_specs=[hbm()] * 5 + [vmem(), vmem()],
        out_specs=[vmem()] * 3,
        scratch_shapes=[
            pltpu.VMEM((2 * tokens, 2 * HEAD_SIZE), queries.dtype),
            pltpu.VMEM((tokens, cols), queries.dtype),
            *small(scalars),
            pltpu.SemaphoreType.DMA((5,)),
        ],
        compiler_params=pltpu.CompilerParams(vmem_limit_bytes=16 << 20),
        cost_estimate=pl.CostEstimate(
            flops=4 * tokens * cols * 640 * 3, transcendentals=tokens * heads * 640, bytes_accessed=4 * tokens * cols
        ),
    )(*[stay(a) for a in scalars], stay(queries), prev, local)


def far_body(
    offsets_hbm, unions_hbm, picks_hbm, counts_hbm, q_hbm, sum_ref, peak_ref, total_ref, prev_ref, same_ref, other_ref, out_ref, far,
    q_ref, offsets_ref, unions, picks, counts, sem,
    *, group, heads, per_dev, owners,
):
    rank = lax.axis_index("ctx")
    vper, union = picks.shape[1], unions.shape[1]
    hops = owners // 2 - 1
    slots = [(None, 0, j) for j in range(vper)]
    slots += [(k, side, j) for k in range(hops) for side in range(2) for j in range(vper)]
    extra = len(slots) % 2
    slots += [slots[-1]] * extra
    width = heads * HEAD_SIZE
    load = pltpu.make_async_copy(q_hbm.at[:, pl.ds(group * width, width)], q_ref, sem.at[4])
    load.start()
    tables = [(offsets_hbm, offsets_ref), (unions_hbm, unions), (picks_hbm, picks), (counts_hbm, counts)]
    tables = [pltpu.make_async_copy(a, b, sem.at[i]) for i, (a, b) in enumerate(tables)]
    for copy in tables:
        copy.start()
    lane = lax.broadcasted_iota(jnp.int32, (1, PAIR), 1)
    block_row = lax.broadcasted_iota(jnp.int32, (per_dev, PAIR), 0)

    for copy in tables:
        copy.wait()
    hides = []
    for i in range(heads):
        head = group * heads + i
        goods = []
        for at, slot in enumerate(slots):
            k, side, j = slot
            owner = rank - 1 if k is None else (rank ^ 1 if side else rank) - 2 * (k + 1)
            good = (owner >= 0) & (owner <= rank - (1 if k is None else 2))
            owner = jnp.maximum(owner, 0)
            entry, used = picked(picks, counts, head, owner, j)
            good = good & used
            if extra and at == len(slots) - 1:
                good = good & False
            if k is None:
                source = prev_ref
                block = unions[group, entry, owner]
                distance = block_row + (per_dev - block)
                seen = jnp.full((per_dev, PAIR), 1.0)
                for s in range(offsets_ref.shape[0]):
                    seen = jnp.where(distance == offsets_ref[s, head], 0.0, seen)
                bias = jnp.where(seen * jnp.where(good, 1.0, 0.0) > 0.5, 0.0, HIDE)
                start = block * BLOCK
            else:
                source = other_ref if side else same_ref
                bias = jnp.where(good, 0.0, HIDE).astype(jnp.float32)
                start = (k * union + entry) * BLOCK
            goods.append(bias)
            far[i, pl.ds(at * BLOCK, BLOCK), :] = source[pl.ds(pl.multiple_of(start, BLOCK), BLOCK), :]
        masks = []
        for tile in range(len(slots) // 2):
            mask = jnp.where(lane < BLOCK, goods[2 * tile], goods[2 * tile + 1])
            if mask.shape[0] > 1:
                mask = jnp.concatenate(
                    [jnp.broadcast_to(mask[r : r + 1], (BLOCK, PAIR)) for r in range(per_dev)], axis=0
                )
            masks.append(mask)
        hides.append(masks)

    def scores_of(i):
        return lax.dot_general(
            q_ref[:, i * HEAD_SIZE : (i + 1) * HEAD_SIZE], far[i, :, :HEAD_SIZE], CONTRACT,
            preferred_element_type=jnp.float32,
        )

    load.wait()
    ahead = scores_of(0)
    for i in range(heads):
        cols = slice(i * HEAD_SIZE, (i + 1) * HEAD_SIZE)
        scores = ahead
        if i + 1 < heads:
            ahead = scores_of(i + 1)
        tiles = [scores[:, t * PAIR : (t + 1) * PAIR] + mask for t, mask in enumerate(hides[i])]
        before = peak_ref[:, cols]
        highest = functools.reduce(jnp.maximum, tiles)
        peak = jnp.maximum(jnp.max(highest, axis=1, keepdims=True), before)
        weights = [jnp.exp2((tile - peak) * SCALE2) for tile in tiles]
        keep = jnp.exp2((before - peak) * SCALE2)
        total = jnp.sum(functools.reduce(jnp.add, weights), axis=1, keepdims=True) + keep * total_ref[:, cols]
        numer = jnp.dot(
            jnp.concatenate([w.astype(jnp.bfloat16) for w in weights], axis=1), far[i, :, HEAD_SIZE:],
            preferred_element_type=jnp.float32,
        )
        out_ref[:, cols] = ((numer + keep * sum_ref[:, cols]) / total).astype(out_ref.dtype)


def attend_far(scalars, queries, sums, peaks, totals, prev, same, other, group, heads, owners):
    tokens = queries.shape[0]
    cols = heads * HEAD_SIZE
    slots = (owners - 1) * scalars[2].shape[1]
    slots += slots % 2
    per_dev = tokens // BLOCK
    return pl.pallas_call(
        functools.partial(far_body, group=group, heads=heads, per_dev=per_dev, owners=owners),
        out_shape=jax.ShapeDtypeStruct((tokens, cols), queries.dtype),
        in_specs=[hbm()] * 5 + [vmem()] * 6,
        out_specs=vmem(),
        scratch_shapes=[
            pltpu.VMEM((heads, slots * BLOCK, 2 * HEAD_SIZE), queries.dtype),
            pltpu.VMEM((tokens, cols), queries.dtype),
            *small(scalars),
            pltpu.SemaphoreType.DMA((5,)),
        ],
        compiler_params=pltpu.CompilerParams(vmem_limit_bytes=24 << 20),
        cost_estimate=pl.CostEstimate(
            flops=4 * tokens * cols * 512 * 3, transcendentals=tokens * heads * 512, bytes_accessed=4 * tokens * cols
        ),
    )(*[stay(a) for a in scalars], stay(queries), sums, peaks, totals, prev, same, other)


def project_body(*refs, spots, has_sum, groups):
    count = len(spots)
    ins, weight = refs[:count], refs[count]
    out = refs[-1]
    seat, members = lax.axis_index("head"), lax.axis_size("head")
    depth = ins[0].shape[1]
    total = refs[count + 1][...] if has_sum else None
    for x, (flip, by, g) in zip(ins, spots):
        source = lax.rem((seat ^ 1 if flip else seat) + members - by, members)
        start = pl.multiple_of((source * groups + g) * depth, depth)
        part = jnp.dot(x[...], weight[pl.ds(start, depth), :], preferred_element_type=jnp.float32)
        total = part if total is None else total + part
    out[...] = total.astype(out.dtype)


def project(ins, spots, weight, sums, dtype, groups):
    tokens, depth = ins[0].shape
    cols = weight.shape[1]
    args = list(ins) + [weight] + ([] if sums is None else [sums])
    return pl.pallas_call(
        functools.partial(project_body, spots=spots, has_sum=sums is not None, groups=groups),
        in_specs=[vmem()] * len(args),
        out_specs=vmem(),
        out_shape=jax.ShapeDtypeStruct((tokens, cols), dtype),
        compiler_params=pltpu.CompilerParams(vmem_limit_bytes=24 << 20),
        cost_estimate=pl.CostEstimate(
            flops=2 * tokens * cols * depth * len(ins) * 2, transcendentals=0, bytes_accessed=2 * depth * cols * len(ins)
        ),
    )(*args)


def turn(array, axis, by):
    size = lax.axis_size(axis)
    return lax.ppermute(array, axis, [(i, (i + by) % size) for i in range(size)])


def onward(array, axis, by):
    size = lax.axis_size(axis)
    return lax.ppermute(array, axis, [(i, i + by) for i in range(size - by)])


def swap(array, axis):
    size = lax.axis_size(axis)
    return lax.ppermute(array, axis, [(i, i ^ 1) for i in range(size)])


def shards(
    queries, key_rows, value_rows, slash_offsets, union_blocks, head_picks, owner_counts, out_weight
):
    groups = key_rows.shape[1] // HEAD_SIZE
    owners, members = lax.axis_size("ctx"), lax.axis_size("head")
    heads = slash_offsets.shape[0] // groups
    unions = jnp.transpose(union_blocks, (0, 2, 1))
    picks = jnp.transpose(head_picks, (0, 2, 1))
    scalars = (slash_offsets.T, unions, picks, owner_counts)
    made = prep(unions, key_rows, value_rows, groups, union_blocks.shape[2])
    joined, blocks, both = made[:groups], made[groups : 2 * groups], made[2 * groups]
    hops = owners // 2 - 1
    prevs, near, sames, others = [], [], [], []
    if hops > 0:
        longest = onward(both, "ctx", 2 * hops)
    for g in range(groups):
        span = blocks[g].shape[0]
        arrived = [longest[g * span : (g + 1) * span]] if hops > 0 else []
        for k in reversed(range(hops - 1)):
            arrived.append(onward(blocks[g], "ctx", 2 * (k + 1)))
        prevs.append(onward(joined[g], "ctx", 1))
        if hops > 0:
            sames.append(jnp.concatenate(arrived[::-1], axis=0))
            others.append(swap(sames[g], "ctx"))
        else:
            sames.append(blocks[g])
            others.append(blocks[g])
    for g in range(groups):
        near.append(attend_near(scalars, queries, prevs[g], joined[g], g, heads))
    done, mates = [], []
    for g in range(groups):
        done.append(attend_far(scalars, queries, *near[g], prevs[g], sames[g], others[g], g, heads, owners))
        mates.append(swap(done[g], "head"))
    sums = None
    crossed = []
    for by in range(2, members, 2):
        for g in range(groups):
            here = turn(done[g], "head", by)
            crossed.append((here, swap(here, "head"), by, g))
    for g in range(groups):
        only = not crossed and g == groups - 1
        sums = project(
            [done[g], mates[g]], [(False, 0, g), (True, 0, g)], out_weight, sums,
            jnp.bfloat16 if only else jnp.float32, groups,
        )
    for at, (here, there, by, g) in enumerate(crossed):
        last = at == len(crossed) - 1
        sums = project([here], [(False, by, g)], out_weight, sums, jnp.float32, groups)
        sums = project([there], [(True, by, g)], out_weight, sums, jnp.bfloat16 if last else jnp.float32, groups)
    return sums


def solution(mesh):
    in_specs = (
        P("ctx", "head"),
        P("ctx", "head"),
        P("ctx", "head"),
        P("head", None),
        P("head", None, None),
        P("head", None, None),
        P("head", None),
        P(None, "head"),
    )
    return jax.shard_map(shards, mesh=mesh, in_specs=in_specs, out_specs=P("ctx", "head"), check_vma=False)
```
